32 devices in a mesh: pts: 8 (over y, x, core), cand: 4 (over z).
Axes of the slice: x: 2, y: 2, z: 4, core: 2. Of those that a mesh axis runs over, the one named last changes fastest.
Arguments:
- points: bfloat16 [8192, 1024], P('pts'), may hold values from -6 to 6
- weights: float32 [8192], P('pts'), may hold values from 0.5 to 5
- coverage: float32 [8192], P('pts'), may hold values from -0.5 to 1
- candidates: bfloat16 [4096, 1024], P('cand'), may hold values from -6 to 6
- picks: int32 [64], replicated, may hold values from 0 to 4095
Outputs:
- gains: float32 [4096], P('cand')
- top_gains: float32 [64], replicated
- new_coverage: float32 [8192], P('pts')
The draws below stay inside these ranges and needn't reach their ends.
All inputs are finite; a program needn't handle non-finite values.
Results may differ from the reference program's by a relative error of at most 0.0003.
Values may be sent and summed in bfloat16 or wider, within the bound.
A program may use at most 64 MiB of HBM per device.

```python
import math
import jax
import jax.numpy as jnp
from jax import lax

D = 1024
CAND_DEV = 1024
NPICK = 64
TOPK = 64
NPTS = 8192
NCAND = 4096
N_CAND = 4


def set_ends(result, rng, smallest, top_value):
    dims = result.shape
    place = [jax.random.randint(jax.random.fold_in(rng, axis), (), 0, dims[axis]) for axis in range(len(dims))]
    result = result.at[tuple(place)].set(smallest)
    longest = dims.index(max(dims))
    place[longest] = (place[longest] + 1) % dims[longest]
    return result.at[tuple(place)].set(top_value)


def block_levels(stream_key, dims, shards, smallest, largest):
    def one(position, parts):
        heights = jax.random.uniform(jax.random.fold_in(jax.random.fold_in(stream_key, 6), position), (parts,), jnp.float32, smallest / len(shards), largest / len(shards))
        return jnp.repeat(jnp.exp(heights), dims[position] // parts).reshape((-1,) + (1,) * (len(dims) - position - 1))

    gain = one(*shards[0])
    for cut in shards[1:]:
        gain = gain * one(*cut)
    return gain


def noise(key, shape, width, most, shards=(), dtype=jnp.bfloat16):
    entries = jax.random.normal(key, shape, jnp.float32) * width
    if len(shards) > 0:
        entries = block_levels(key, shape, shards, -0.22, 0.18) * entries
    return jnp.clip(entries, min=-most, max=most).astype(dtype)


def setup_inputs(seed: int = 0) -> dict:
    key_of = jax.random.split(jax.random.key(seed), 6)
    return {
        "points": noise(key_of[0], (NPTS, D), 1.0, 6.0, ((0, 8),)),
        "weights": jnp.clip(jnp.exp(math.log(5.0) - 2.3025851 * jax.random.uniform(key_of[1], (NPTS,), jnp.float32) ** block_levels(key_of[1], (NPTS,), ((0, 8),), -0.2, 0.2)), 0.5, 5.0),
        "coverage": jnp.clip(-0.5 + 1.5 * jax.random.uniform(key_of[2], (NPTS,), jnp.float32) ** block_levels(key_of[2], (NPTS,), ((0, 8),), -0.2, 0.2), -0.5, 1.0),
        "candidates": noise(key_of[3], (NCAND, D), 1.0, 6.0, ((0, 4),)),
        "picks": set_ends(jax.random.randint(key_of[4], (NPICK,), 0, NCAND), jax.random.fold_in(key_of[4], 1), 0, NCAND - 1).astype(jnp.int32),
    }


def reference(points, weights, coverage, candidates, picks):
    scale = D ** -0.5
    total = points.shape[0]
    blocks = candidates.reshape(N_CAND, CAND_DEV, D)

    def block_gain(block):
        sims = jnp.dot(points, block.T, preferred_element_type=jnp.float32) * scale
        return jnp.sum(weights[:, None] * jnp.maximum(sims - coverage[:, None], 0.0), axis=0) / total

    gains = lax.map(block_gain, blocks).reshape(-1)
    top_gains = lax.top_k(gains, TOPK)[0]
    picked = jnp.take(candidates, picks.astype(jnp.int32), axis=0)
    picked_sims = jnp.dot(points, picked.T, preferred_element_type=jnp.float32) * scale
    new_coverage = jnp.maximum(coverage, jnp.max(picked_sims, axis=1))
    return gains, top_gains, new_coverage
```

```python
import functools

import jax
import jax.numpy as jnp
from jax import lax
from jax.experimental import pallas as pl
from jax.experimental.pallas import tpu as pltpu
from jax.sharding import PartitionSpec as P

TOPK = 64
LANES = 128
MESH = pl.DeviceIdType.MESH
F32 = jnp.float32
LOW = -1e30
HIGH = 3e38
CHUNK = 256


def column_tile(row):
    return jnp.transpose(jnp.broadcast_to(row, (LANES, LANES)))


def ranked(columns, rows, count):
    wide = [jnp.broadcast_to(row, (8, LANES)) for row in rows]
    above = [jnp.zeros((8, LANES), F32) for _ in rows]
    for column in columns:
        for g in range(column.shape[0] // 8):
            value = column[g * 8 : (g + 1) * 8, :]
            above = [a + jnp.where(value > w, 1.0, 0.0) for a, w in zip(above, wide)]
    place = lax.broadcasted_iota(jnp.int32, (count, LANES), 0).astype(F32)
    best = jnp.full((count, LANES), HIGH, F32)
    for a, row in zip(above, rows):
        total = jnp.sum(a, axis=0, keepdims=True)
        best = jnp.minimum(best, jnp.where(total <= place, row, HIGH))
    return jnp.min(best, axis=1, keepdims=True)


def as_row(column):
    count = column.shape[0]
    wide = jnp.broadcast_to(column, (count, LANES))
    if count < LANES:
        wide = jnp.concatenate([wide, jnp.full((LANES - count, LANES), -1.0, F32)], axis=0)
    return jnp.transpose(wide)[0:1, :]


def kernel(
    n_pts, n_cand, points, weights, coverage, candidates, picks, gains_out, top_out, cover_out,
    p_buf, c_buf, w_buf, v_buf, k_buf, w_col, v_col, g_acc, b_acc, part, parts, best, bests,
    top, tops, g_col, gains_buf, top_buf, cover_buf,
    in_sem, small_sem, out_sem, part_send, part_recv, best_send, best_recv, top_send, top_recv,
):
    rows, depth = points.shape
    cands = candidates.shape[0]
    me, mz = lax.axis_index("pts"), lax.axis_index("cand")
    n_p, n_c = rows // CHUNK, cands // CHUNK
    tiles_p, tiles_c = rows // LANES, cands // LANES
    scale = depth ** (-0.5)

    small = [
        pltpu.make_async_copy(weights, w_buf, small_sem.at[0]),
        pltpu.make_async_copy(coverage, v_buf, small_sem.at[1]),
        pltpu.make_async_copy(picks, k_buf, small_sem.at[2]),
    ]
    for copy in small:
        copy.start()
    loads = {}
    order = []
    for i in range(max(n_p, n_c)):
        if i < n_c:
            order.append(("c", i))
        if i < n_p:
            order.append(("p", i))
    for at, (kind, i) in enumerate(order):
        src, dst = (points, p_buf) if kind == "p" else (candidates, c_buf)
        span = pl.ds(i * CHUNK, CHUNK)
        loads[kind, i] = pltpu.make_async_copy(src.at[span, :], dst.at[span, :], in_sem.at[at])
        loads[kind, i].start()

    barrier = pltpu.get_barrier_semaphore()
    for k in range(1, n_pts):
        pl.semaphore_signal(
            barrier, inc=1, device_id={"pts": lax.rem(me + k, n_pts)}, device_id_type=MESH
        )
    for k in range(1, n_cand):
        pl.semaphore_signal(
            barrier, inc=1, device_id={"cand": lax.rem(mz + k, n_cand)}, device_id_type=MESH
        )

    for copy in small:
        copy.wait()
    column = mz * cands + lax.broadcasted_iota(jnp.int32, (tiles_c, LANES), 0) * LANES
    column = column + lax.broadcasted_iota(jnp.int32, (tiles_c, LANES), 1)
    chosen = jnp.zeros((tiles_c, LANES), jnp.bool_)
    for k in range(picks.shape[0]):
        chosen = chosen | (column == k_buf[k])
    penalty = jnp.where(chosen, 0.0, LOW)
    w_row = w_buf[...] * (scale / (rows * n_pts))
    v_row = v_buf[...] * (1.0 / scale)
    for t in range(tiles_p):
        w_col[t * LANES : (t + 1) * LANES, :] = column_tile(w_row[t : t + 1, :])
        v_col[t * LANES : (t + 1) * LANES, :] = column_tile(v_row[t : t + 1, :])

    def block(pi, ci):
        ps = pl.ds(pi * CHUNK, CHUNK)
        sims = lax.dot_general(
            p_buf[ps, :], c_buf[pl.ds(ci * CHUNK, CHUNK), :],
            (((1,), (1,)), ((), ())), preferred_element_type=F32,
        )
        w, v = w_col[ps, :], v_col[ps, :]
        found = None
        for l in range(CHUNK // LANES):
            tile = ci * (CHUNK // LANES) + l
            x = sims[:, l * LANES : (l + 1) * LANES]
            value = jnp.maximum(x - v, 0.0) * w
            value = jnp.sum(value.reshape(CHUNK // 8, 8, LANES), axis=0)
            lanes = slice(tile * LANES, (tile + 1) * LANES)
            if pi == 0:
                g_acc[:, lanes] = value
            else:
                g_acc[:, lanes] += value
            x = x + penalty[tile : tile + 1, :]
            found = x if found is None else jnp.maximum(found, x)
        if ci == 0:
            b_acc[ps, :] = found
        else:
            b_acc[ps, :] = jnp.maximum(b_acc[ps, :], found)

    here_p, here_c = [], []
    for kind, i in order:
        loads[kind, i].wait()
        if kind == "p":
            here_p.append(i)
            for ci in here_c:
                block(i, ci)
        else:
            here_c.append(i)
            for pi in here_p:
                block(pi, i)

    for t in range(tiles_c):
        part[t : t + 1, :] = jnp.sum(g_acc[:, t * LANES : (t + 1) * LANES], axis=0, keepdims=True)

    pl.semaphore_wait(barrier, n_pts - 1 + n_cand - 1)

    def exchange(axis, n, mine, src, slots, send, recv):
        for k in range(1, n):
            pltpu.make_async_remote_copy(
                src_ref=src, dst_ref=slots.at[mine], send_sem=send.at[k], recv_sem=recv.at[mine],
                device_id={axis: lax.rem(mine + k, n)}, device_id_type=MESH,
            ).start()

    def arrive(axis, n, mine, src, slots, send, recv):
        for k in range(1, n):
            other = lax.rem(mine + k, n)
            pltpu.make_async_remote_copy(
                src_ref=src, dst_ref=slots.at[other], send_sem=send.at[k], recv_sem=recv.at[other],
                device_id={axis: other}, device_id_type=MESH,
            ).wait()

    exchange("pts", n_pts, me, part, parts, part_send, part_recv)
    parts[me] = part[...]

    for t in range(tiles_p):
        turned = jnp.transpose(b_acc[t * LANES : (t + 1) * LANES, :])
        best[t : t + 1, :] = jnp.max(turned, axis=0, keepdims=True)
    exchange("cand", n_cand, mz, best, bests, best_send, best_recv)

    arrive("pts", n_pts, me, part, parts, part_send, part_recv)
    gains = parts[0]
    for k in range(1, n_pts):
        gains = gains + parts[k]
    gains_buf[...] = gains
    gains_copy = pltpu.make_async_copy(gains_buf, gains_out, out_sem.at[0])
    gains_copy.start()

    for t in range(tiles_c):
        g_col[t * LANES : (t + 1) * LANES, :] = column_tile(gains[t : t + 1, :])
    sorted_col = ranked([g_col], [gains[t : t + 1, :] for t in range(tiles_c)], TOPK)
    top_row = as_row(sorted_col)
    top[...] = top_row
    exchange("cand", n_cand, mz, top, tops, top_send, top_recv)
    tops[mz] = top_row

    arrive("cand", n_cand, mz, best, bests, best_send, best_recv)
    cover = best[...]
    for k in range(1, n_cand):
        cover = jnp.maximum(cover, bests[lax.rem(mz + k, n_cand)])
    cover_buf[...] = jnp.maximum(v_buf[...], cover * scale)
    cover_copy = pltpu.make_async_copy(cover_buf, cover_out, out_sem.at[1])
    cover_copy.start()

    arrive("cand", n_cand, mz, top, tops, top_send, top_recv)
    lists = [tops[k] for k in range(n_cand)]
    merged = ranked([column_tile(row)[:TOPK, :] for row in lists], lists, TOPK)
    top_buf[...] = as_row(merged)[:, :TOPK]
    top_copy = pltpu.make_async_copy(top_buf, top_out, out_sem.at[2])
    top_copy.start()
    gains_copy.wait()
    cover_copy.wait()
    top_copy.wait()


def solution(mesh):
    n_pts, n_cand = mesh.shape["pts"], mesh.shape["cand"]

    def on_device(points, weights, coverage, candidates, picks):
        rows, depth = points.shape
        cands = candidates.shape[0]
        tp, tc = rows // LANES, cands // LANES
        anywhere = pl.BlockSpec(memory_space=pl.ANY)
        dma = pltpu.SemaphoreType.DMA
        vmem = pltpu.VMEM
        gains, top, cover = pl.pallas_call(
            functools.partial(kernel, n_pts, n_cand),
            out_shape=(
                jax.ShapeDtypeStruct((tc, LANES), F32),
                jax.ShapeDtypeStruct((1, TOPK), F32),
                jax.ShapeDtypeStruct((tp, LANES), F32),
            ),
            in_specs=[anywhere] * 5,
            out_specs=(anywhere,) * 3,
            scratch_shapes=[
                vmem((rows, depth), points.dtype), vmem((cands, depth), candidates.dtype),
                vmem((tp, LANES), F32), vmem((tp, LANES), F32),
                pltpu.SMEM(picks.shape, jnp.int32),
                vmem((rows, LANES), F32), vmem((rows, LANES), F32),
                vmem((8, cands), F32), vmem((rows, LANES), F32),
                vmem((tc, LANES), F32), vmem((n_pts, tc, LANES), F32),
                vmem((tp, LANES), F32), vmem((n_cand, tp, LANES), F32),
                vmem((1, LANES), F32), vmem((n_cand, 1, LANES), F32),
                vmem((cands, LANES), F32),
                vmem((tc, LANES), F32), vmem((1, TOPK), F32), vmem((tp, LANES), F32),
                dma((rows // CHUNK + cands // CHUNK,)), dma((3,)), dma((3,)),
                dma((n_pts,)), dma((n_pts,)),
                dma((n_cand,)), dma((n_cand,)),
                dma((n_cand,)), dma((n_cand,)),
            ],
            compiler_params=pltpu.CompilerParams(
                collective_id=0, has_side_effects=True, vmem_limit_bytes=60 * 2**20
            ),
            name="facility",
        )(points, weights.reshape(tp, LANES), coverage.reshape(tp, LANES), candidates, picks)
        return gains.reshape(cands), top.reshape(TOPK), cover.reshape(rows)

    placed = (P("pts", None), P("pts"), P("pts"), P("cand", None), P())
    return jax.shard_map(
        on_device, mesh=mesh, in_specs=placed, out_specs=(P("cand"), P(), P("pts")), check_vma=False
    )
```

```python
import functools

import jax
import jax.numpy as jnp
from jax import lax
from jax.experimental import pallas as pl
from jax.experimental.pallas import tpu as pltpu
from jax.sharding import PartitionSpec as P

TOPK = 64
LANES = 128
MESH = pl.DeviceIdType.MESH
F32 = jnp.float32
LOW = -1e30
HIGH = 3e38
CHUNK = 256


def column_tile(row):
    return jnp.transpose(jnp.broadcast_to(row, (LANES, LANES)))


def ranked(columns, rows, count):
    wide = [jnp.broadcast_to(row, (8, LANES)) for row in rows]
    above = [jnp.zeros((8, LANES), F32) for _ in rows]
    for column in columns:
        for g in range(column.shape[0] // 8):
            value = column[g * 8 : (g + 1) * 8, :]
            above = [a + jnp.where(value > w, 1.0, 0.0) for a, w in zip(above, wide)]
    place = lax.broadcasted_iota(jnp.int32, (count, LANES), 0).astype(F32)
    best = jnp.full((count, LANES), HIGH, F32)
    for a, row in zip(above, rows):
        total = jnp.sum(a, axis=0, keepdims=True)
        best = jnp.minimum(best, jnp.where(total <= place, row, HIGH))
    return jnp.min(best, axis=1, keepdims=True)


def as_row(column):
    count = column.shape[0]
    wide = jnp.broadcast_to(column, (count, LANES))
    if count < LANES:
        wide = jnp.concatenate([wide, jnp.full((LANES - count, LANES), -1.0, F32)], axis=0)
    return jnp.transpose(wide)[0:1, :]


def kernel(
    n_pts, n_cand, points, weights, coverage, candidates, picks, gains_out, lists_out, cover_out,
    p_buf, c_buf, w_buf, v_buf, k_buf, w_col, v_col, g_acc, b_acc, part, parts, best, bests,
    top, tops, g_col, in_sem, small_sem, part_send, part_recv, best_send, best_recv, top_send, top_recv,
):
    rows, depth = points.shape
    cands = candidates.shape[0]
    me, mz = lax.axis_index("pts"), lax.axis_index("cand")
    n_p, n_c = rows // CHUNK, cands // CHUNK
    tiles_p, tiles_c = rows // LANES, cands // LANES
    scale = depth ** (-0.5)

    small = [
        pltpu.make_async_copy(weights, w_buf, small_sem.at[0]),
        pltpu.make_async_copy(coverage, v_buf, small_sem.at[1]),
        pltpu.make_async_copy(picks, k_buf, small_sem.at[2]),
    ]
    for copy in small:
        copy.start()
    loads = {}
    order = []
    for i in range(max(n_p, n_c)):
        if i < n_c:
            order.append(("c", i))
        if i < n_p:
            order.append(("p", i))
    for at, (kind, i) in enumerate(order):
        src, dst = (points, p_buf) if kind == "p" else (candidates, c_buf)
        span = pl.ds(i * CHUNK, CHUNK)
        loads[kind, i] = pltpu.make_async_copy(src.at[span, :], dst.at[span, :], in_sem.at[at])
        loads[kind, i].start()

    barrier = pltpu.get_barrier_semaphore()
    for k in range(1, n_pts):
        pl.semaphore_signal(
            barrier, inc=1, device_id={"pts": lax.rem(me + k, n_pts)}, device_id_type=MESH
        )
    for k in range(1, n_cand):
        pl.semaphore_signal(
            barrier, inc=1, device_id={"cand": lax.rem(mz + k, n_cand)}, device_id_type=MESH
        )

    for copy in small:
        copy.wait()
    column = mz * cands + lax.broadcasted_iota(jnp.int32, (tiles_c, LANES), 0) * LANES
    column = column + lax.broadcasted_iota(jnp.int32, (tiles_c, LANES), 1)
    chosen = jnp.zeros((tiles_c, LANES), jnp.bool_)
    for k in range(picks.shape[0]):
        chosen = chosen | (column == k_buf[k])
    penalty = jnp.where(chosen, 0.0, LOW)
    w_row = w_buf[...] * (scale / (rows * n_pts))
    v_row = v_buf[...] * (1.0 / scale)
    for t in range(tiles_p):
        w_col[t * LANES : (t + 1) * LANES, :] = column_tile(w_row[t : t + 1, :])
        v_col[t * LANES : (t + 1) * LANES, :] = column_tile(v_row[t : t + 1, :])

    def block(pi, ci):
        ps = pl.ds(pi * CHUNK, CHUNK)
        sims = lax.dot_general(
            p_buf[ps, :], c_buf[pl.ds(ci * CHUNK, CHUNK), :],
            (((1,), (1,)), ((), ())), preferred_element_type=F32,
        )
        w, v = w_col[ps, :], v_col[ps, :]
        found = None
        for l in range(CHUNK // LANES):
            tile = ci * (CHUNK // LANES) + l
            x = sims[:, l * LANES : (l + 1) * LANES]
            value = jnp.maximum(x - v, 0.0) * w
            value = jnp.sum(value.reshape(CHUNK // 8, 8, LANES), axis=0)
            lanes = slice(tile * LANES, (tile + 1) * LANES)
            if pi == 0:
                g_acc[:, lanes] = value
            else:
                g_acc[:, lanes] += value
            x = x + penalty[tile : tile + 1, :]
            found = x if found is None else jnp.maximum(found, x)
        if ci == 0:
            b_acc[ps, :] = found
        else:
            b_acc[ps, :] = jnp.maximum(b_acc[ps, :], found)

    here_p, here_c = [], []
    for kind, i in order:
        loads[kind, i].wait()
        if kind == "p":
            here_p.append(i)
            for ci in here_c:
                block(i, ci)
        else:
            here_c.append(i)
            for pi in here_p:
                block(pi, i)

    for t in range(tiles_c):
        part[t : t + 1, :] = jnp.sum(g_acc[:, t * LANES : (t + 1) * LANES], axis=0, keepdims=True)

    pl.semaphore_wait(barrier, n_pts - 1 + n_cand - 1)

    def exchange(axis, n, mine, src, slots, send, recv):
        for k in range(1, n):
            pltpu.make_async_remote_copy(
                src_ref=src, dst_ref=slots.at[mine], send_sem=send.at[k], recv_sem=recv.at[mine],
                device_id={axis: lax.rem(mine + k, n)}, device_id_type=MESH,
            ).start()

    def arrive(axis, n, mine, src, slots, send, recv):
        for k in range(1, n):
            other = lax.rem(mine + k, n)
            pltpu.make_async_remote_copy(
                src_ref=src, dst_ref=slots.at[other], send_sem=send.at[k], recv_sem=recv.at[other],
                device_id={axis: other}, device_id_type=MESH,
            ).wait()

    exchange("pts", n_pts, me, part, parts, part_send, part_recv)
    parts[me] = part[...]

    for t in range(tiles_p):
        turned = jnp.transpose(b_acc[t * LANES : (t + 1) * LANES, :])
        best[t : t + 1, :] = jnp.max(turned, axis=0, keepdims=True)
    exchange("cand", n_cand, mz, best, bests, best_send, best_recv)

    arrive("pts", n_pts, me, part, parts, part_send, part_recv)
    gains = parts[0]
    for k in range(1, n_pts):
        gains = gains + parts[k]
    gains_out[...] = gains

    for t in range(tiles_c):
        g_col[t * LANES : (t + 1) * LANES, :] = column_tile(gains[t : t + 1, :])
    sorted_col = ranked([g_col], [gains[t : t + 1, :] for t in range(tiles_c)], TOPK)
    top_row = as_row(sorted_col)
    top[...] = top_row
    exchange("cand", n_cand, mz, top, tops, top_send, top_recv)
    tops[mz] = top_row

    arrive("cand", n_cand, mz, best, bests, best_send, best_recv)
    cover = best[...]
    for k in range(1, n_cand):
        cover = jnp.maximum(cover, bests[lax.rem(mz + k, n_cand)])
    cover_out[...] = jnp.maximum(v_buf[...], cover * scale)

    arrive("cand", n_cand, mz, top, tops, top_send, top_recv)
    for k in range(n_cand):
        lists_out[k : k + 1, :] = tops[k]


def finish(gains, lists, cover, gains_out, top_out, cover_out, sems, top_buf):
    gains_copy = pltpu.make_async_copy(gains, gains_out, sems.at[0])
    cover_copy = pltpu.make_async_copy(cover, cover_out, sems.at[1])
    gains_copy.start()
    cover_copy.start()
    rows = [lists[k : k + 1, :] for k in range(lists.shape[0])]
    merged = ranked([column_tile(row)[:TOPK, :] for row in rows], rows, TOPK)
    top_buf[...] = as_row(merged)[:, :TOPK]
    top_copy = pltpu.make_async_copy(top_buf, top_out, sems.at[2])
    top_copy.start()
    gains_copy.wait()
    cover_copy.wait()
    top_copy.wait()


def solution(mesh):
    n_pts, n_cand = mesh.shape["pts"], mesh.shape["cand"]

    def on_device(points, weights, coverage, candidates, picks):
        rows, depth = points.shape
        cands = candidates.shape[0]
        tp, tc = rows // LANES, cands // LANES
        anywhere = pl.BlockSpec(memory_space=pl.ANY)
        dma = pltpu.SemaphoreType.DMA
        vmem = pltpu.VMEM
        gains, lists, cover = pl.pallas_call(
            functools.partial(kernel, n_pts, n_cand),
            out_shape=(
                vmem((tc, LANES), F32),
                vmem((n_cand, LANES), F32),
                vmem((tp, LANES), F32),
            ),
            in_specs=[anywhere] * 5,
            out_specs=(pl.BlockSpec(memory_space=vmem),) * 3,
            scratch_shapes=[
                vmem((rows, depth), points.dtype), vmem((cands, depth), candidates.dtype),
                vmem((tp, LANES), F32), vmem((tp, LANES), F32),
                pltpu.SMEM(picks.shape, jnp.int32),
                vmem((rows, LANES), F32), vmem((rows, LANES), F32),
                vmem((8, cands), F32), vmem((rows, LANES), F32),
                vmem((tc, LANES), F32), vmem((n_pts, tc, LANES), F32),
                vmem((tp, LANES), F32), vmem((n_cand, tp, LANES), F32),
                vmem((1, LANES), F32), vmem((n_cand, 1, LANES), F32),
                vmem((cands, LANES), F32),
                dma((rows // CHUNK + cands // CHUNK,)), dma((3,)),
                dma((n_pts,)), dma((n_pts,)),
                dma((n_cand,)), dma((n_cand,)),
                dma((n_cand,)), dma((n_cand,)),
            ],
            compiler_params=pltpu.CompilerParams(
                collective_id=0, has_side_effects=True, vmem_limit_bytes=60 * 2**20
            ),
            name="facility",
        )(points, weights.reshape(tp, LANES), coverage.reshape(tp, LANES), candidates, picks)
        gains, top, cover = pl.pallas_call(
            finish,
            out_shape=(
                jax.ShapeDtypeStruct((tc, LANES), F32),
                jax.ShapeDtypeStruct((1, TOPK), F32),
                jax.ShapeDtypeStruct((tp, LANES), F32),
            ),
            in_specs=[pl.BlockSpec(memory_space=vmem)] * 3,
            out_specs=(anywhere,) * 3,
            scratch_shapes=[dma((3,)), vmem((1, TOPK), F32)],
            name="finish",
        )(*(pltpu.with_memory_space_constraint(x, vmem) for x in (gains, lists, cover)))
        return gains.reshape(cands), top.reshape(TOPK), cover.reshape(rows)

    placed = (P("pts", None), P("pts"), P("pts"), P("cand", None), P())
    return jax.shard_map(
        on_device, mesh=mesh, in_specs=placed, out_specs=(P("cand"), P(), P("pts")), check_vma=False
    )
```

```python
import functools

import jax
import jax.numpy as jnp
from jax import lax
from jax.experimental import pallas as pl
from jax.experimental.pallas import tpu as pltpu
from jax.sharding import PartitionSpec as P

TOPK = 64
LANES = 128
MESH = pl.DeviceIdType.MESH
F32 = jnp.float32
LOW = -1e30
HIGH = 3e38
CHUNK = 256


def column_tile(row):
    return jnp.transpose(jnp.broadcast_to(row, (LANES, LANES)))


def ranked(columns, rows, count):
    wide = [jnp.broadcast_to(row, (8, LANES)) for row in rows]
    above = [jnp.zeros((8, LANES), F32) for _ in rows]
    for column in columns:
        for g in range(column.shape[0] // 8):
            value = column[g * 8 : (g + 1) * 8, :]
            above = [a + jnp.where(value > w, 1.0, 0.0) for a, w in zip(above, wide)]
    place = lax.broadcasted_iota(jnp.int32, (count, LANES), 0).astype(F32)
    best = jnp.full((count, LANES), HIGH, F32)
    for a, row in zip(above, rows):
        total = jnp.sum(a, axis=0, keepdims=True)
        best = jnp.minimum(best, jnp.where(total <= place, row, HIGH))
    return jnp.min(best, axis=1, keepdims=True)


def as_row(column):
    count = column.shape[0]
    wide = jnp.broadcast_to(column, (count, LANES))
    if count < LANES:
        wide = jnp.concatenate([wide, jnp.full((LANES - count, LANES), -1.0, F32)], axis=0)
    return jnp.transpose(wide)[0:1, :]


def kernel(
    n_pts, n_cand, points, weights, coverage, candidates, picks, gains_out, lists_out, cover_out,
    p_buf, c_buf, w_buf, v_buf, k_buf, w_col, v_col, g_acc, b_acc, part, parts, best, bests,
    top, tops, g_col, in_sem, small_sem, part_send, part_recv, best_send, best_recv, top_send, top_recv,
):
    rows, depth = points.shape
    cands = candidates.shape[0]
    me, mz = lax.axis_index("pts"), lax.axis_index("cand")
    n_p, n_c = rows // CHUNK, cands // CHUNK
    tiles_p, tiles_c = rows // LANES, cands // LANES
    scale = depth ** (-0.5)

    small = [
        pltpu.make_async_copy(weights, w_buf, small_sem.at[0]),
        pltpu.make_async_copy(coverage, v_buf, small_sem.at[1]),
        pltpu.make_async_copy(picks, k_buf, small_sem.at[2]),
    ]
    for copy in small:
        copy.start()
    barrier = pltpu.get_barrier_semaphore()
    for k in range(1, n_cand):
        pl.semaphore_signal(
            barrier, inc=1, device_id={"cand": lax.rem(mz + k, n_cand)}, device_id_type=MESH
        )

    loads = {}
    order = []
    for i in range(max(n_p, n_c)):
        if i < n_c:
            order.append(("c", i))
        if i < n_p:
            order.append(("p", i))
    for at, (kind, i) in enumerate(order):
        src, dst = (points, p_buf) if kind == "p" else (candidates, c_buf)
        span = pl.ds(i * CHUNK, CHUNK)
        loads[kind, i] = pltpu.make_async_copy(src.at[span, :], dst.at[span, :], in_sem.at[at])
        loads[kind, i].start()

    for k in range(1, n_pts):
        pl.semaphore_signal(
            barrier, inc=1, device_id={"pts": lax.rem(me + k, n_pts)}, device_id_type=MESH
        )

    for copy in small:
        copy.wait()
    column = mz * cands + lax.broadcasted_iota(jnp.int32, (tiles_c, LANES), 0) * LANES
    column = column + lax.broadcasted_iota(jnp.int32, (tiles_c, LANES), 1)
    chosen = jnp.zeros((tiles_c, LANES), jnp.bool_)
    for k in range(picks.shape[0]):
        chosen = chosen | (column == k_buf[k])
    penalty = jnp.where(chosen, 0.0, LOW)
    w_row = w_buf[...] * (scale / (rows * n_pts))
    v_row = v_buf[...] * (1.0 / scale)
    for t in range(tiles_p):
        w_col[t * LANES : (t + 1) * LANES, :] = column_tile(w_row[t : t + 1, :])
        v_col[t * LANES : (t + 1) * LANES, :] = column_tile(v_row[t : t + 1, :])

    def block(p_from, p_to, c_from, c_to):
        ps, many = pl.ds(p_from, p_to - p_from), p_to - p_from
        sims = lax.dot_general(
            p_buf[ps, :], c_buf[pl.ds(c_from, c_to - c_from), :],
            (((1,), (1,)), ((), ())), preferred_element_type=F32,
        )
        w, v = w_col[ps, :], v_col[ps, :]
        found = None
        for tile in range(c_from // LANES, c_to // LANES):
            lanes = slice(tile * LANES, (tile + 1) * LANES)
            x = sims[:, tile * LANES - c_from : (tile + 1) * LANES - c_from]
            value = jnp.maximum(x - v, 0.0) * w
            value = jnp.sum(value.reshape(many // 8, 8, LANES), axis=0)
            if p_from == 0:
                g_acc[:, lanes] = value
            else:
                g_acc[:, lanes] += value
            x = x + penalty[tile : tile + 1, :]
            found = x if found is None else jnp.maximum(found, x)
        if c_from == 0:
            b_acc[ps, :] = found
        else:
            b_acc[ps, :] = jnp.maximum(b_acc[ps, :], found)

    here_p = here_c = 0
    for kind, i in order:
        loads[kind, i].wait()
        if kind == "p":
            here_p += CHUNK
            if here_c:
                block(here_p - CHUNK, here_p, 0, here_c)
        else:
            here_c += CHUNK
            if here_p:
                block(0, here_p, here_c - CHUNK, here_c)

    for t in range(tiles_c):
        part[t : t + 1, :] = jnp.sum(g_acc[:, t * LANES : (t + 1) * LANES], axis=0, keepdims=True)

    pl.semaphore_wait(barrier, n_pts - 1 + n_cand - 1)

    def exchange(axis, n, mine, src, slots, send, recv):
        for k in range(1, n):
            pltpu.make_async_remote_copy(
                src_ref=src, dst_ref=slots.at[mine], send_sem=send.at[k], recv_sem=recv.at[mine],
                device_id={axis: lax.rem(mine + k, n)}, device_id_type=MESH,
            ).start()

    def arrive(axis, n, mine, src, slots, send, recv):
        for k in range(1, n):
            other = lax.rem(mine + k, n)
            pltpu.make_async_remote_copy(
                src_ref=src, dst_ref=slots.at[other], send_sem=send.at[k], recv_sem=recv.at[other],
                device_id={axis: other}, device_id_type=MESH,
            ).wait()

    exchange("pts", n_pts, me, part, parts, part_send, part_recv)
    parts[me] = part[...]

    for t in range(tiles_p):
        turned = jnp.transpose(b_acc[t * LANES : (t + 1) * LANES, :])
        best[t : t + 1, :] = jnp.max(turned, axis=0, keepdims=True)
    exchange("cand", n_cand, mz, best, bests, best_send, best_recv)

    arrive("pts", n_pts, me, part, parts, part_send, part_recv)
    gains = parts[0]
    for k in range(1, n_pts):
        gains = gains + parts[k]
    gains_out[...] = gains

    for t in range(tiles_c):
        g_col[t * LANES : (t + 1) * LANES, :] = column_tile(gains[t : t + 1, :])
    sorted_col = ranked([g_col], [gains[t : t + 1, :] for t in range(tiles_c)], TOPK)
    top_row = as_row(sorted_col)
    top[...] = top_row
    exchange("cand", n_cand, mz, top, tops, top_send, top_recv)
    tops[mz] = top_row

    arrive("cand", n_cand, mz, best, bests, best_send, best_recv)
    cover = best[...]
    for k in range(1, n_cand):
        cover = jnp.maximum(cover, bests[lax.rem(mz + k, n_cand)])
    cover_out[...] = jnp.maximum(v_buf[...], cover * scale)

    arrive("cand", n_cand, mz, top, tops, top_send, top_recv)
    for k in range(n_cand):
        lists_out[k : k + 1, :] = tops[k]


def finish(gains, lists, cover, gains_out, top_out, cover_out, sems, top_buf):
    gains_copy = pltpu.make_async_copy(gains, gains_out, sems.at[0])
    cover_copy = pltpu.make_async_copy(cover, cover_out, sems.at[1])
    gains_copy.start()
    cover_copy.start()
    rows = [lists[k : k + 1, :] for k in range(lists.shape[0])]
    merged = ranked([column_tile(row)[:TOPK, :] for row in rows], rows, TOPK)
    top_buf[...] = as_row(merged)[:, :TOPK]
    top_copy = pltpu.make_async_copy(top_buf, top_out, sems.at[2])
    top_copy.start()
    gains_copy.wait()
    cover_copy.wait()
    top_copy.wait()


def solution(mesh):
    n_pts, n_cand = mesh.shape["pts"], mesh.shape["cand"]

    def on_device(points, weights, coverage, candidates, picks):
        rows, depth = points.shape
        cands = candidates.shape[0]
        tp, tc = rows // LANES, cands // LANES
        anywhere = pl.BlockSpec(memory_space=pl.ANY)
        dma = pltpu.SemaphoreType.DMA
        vmem = pltpu.VMEM
        gains, lists, cover = pl.pallas_call(
            functools.partial(kernel, n_pts, n_cand),
            out_shape=(
                vmem((tc, LANES), F32),
                vmem((n_cand, LANES), F32),
                vmem((tp, LANES), F32),
            ),
            in_specs=[anywhere] * 5,
            out_specs=(pl.BlockSpec(memory_space=vmem),) * 3,
            scratch_shapes=[
                vmem((rows, depth), points.dtype), vmem((cands, depth), candidates.dtype),
                vmem((tp, LANES), F32), vmem((tp, LANES), F32),
                pltpu.SMEM(picks.shape, jnp.int32),
                vmem((rows, LANES), F32), vmem((rows, LANES), F32),
                vmem((8, cands), F32), vmem((rows, LANES), F32),
                vmem((tc, LANES), F32), vmem((n_pts, tc, LANES), F32),
                vmem((tp, LANES), F32), vmem((n_cand, tp, LANES), F32),
                vmem((1, LANES), F32), vmem((n_cand, 1, LANES), F32),
                vmem((cands, LANES), F32),
                dma((rows // CHUNK + cands // CHUNK,)), dma((3,)),
                dma((n_pts,)), dma((n_pts,)),
                dma((n_cand,)), dma((n_cand,)),
                dma((n_cand,)), dma((n_cand,)),
            ],
            compiler_params=pltpu.CompilerParams(
                collective_id=0, has_side_effects=True, vmem_limit_bytes=60 * 2**20
            ),
            name="facility",
        )(points, weights.reshape(tp, LANES), coverage.reshape(tp, LANES), candidates, picks)
        gains, top, cover = pl.pallas_call(
            finish,
            out_shape=(
                jax.ShapeDtypeStruct((tc, LANES), F32),
                jax.ShapeDtypeStruct((1, TOPK), F32),
                jax.ShapeDtypeStruct((tp, LANES), F32),
            ),
            in_specs=[pl.BlockSpec(memory_space=vmem)] * 3,
            out_specs=(anywhere,) * 3,
            scratch_shapes=[dma((3,)), vmem((1, TOPK), F32)],
            name="finish",
        )(*(pltpu.with_memory_space_constraint(x, vmem) for x in (gains, lists, cover)))
        return gains.reshape(cands), top.reshape(TOPK), cover.reshape(rows)

    placed = (P("pts", None), P("pts"), P("pts"), P("cand", None), P())
    return jax.shard_map(
        on_device, mesh=mesh, in_specs=placed, out_specs=(P("cand"), P(), P("pts")), check_vma=False
    )
```

```python
import functools

import jax
import jax.numpy as jnp
from jax import lax
from jax.experimental import pallas as pl
from jax.experimental.pallas import tpu as pltpu
from jax.sharding import PartitionSpec as P

TOPK = 64
LANES = 128
MESH = pl.DeviceIdType.MESH
F32 = jnp.float32
LOW = -1e30
HIGH = 3e38
CHUNK = 256


def column_tile(row):
    return jnp.transpose(jnp.broadcast_to(row, (LANES, LANES)))


def ranked(columns, rows, count):
    wide = [jnp.broadcast_to(row, (8, LANES)) for row in rows]
    above = [jnp.zeros((8, LANES), F32) for _ in rows]
    for column in columns:
        for g in range(column.shape[0] // 8):
            value = column[g * 8 : (g + 1) * 8, :]
            above = [a + jnp.where(value > w, 1.0, 0.0) for a, w in zip(above, wide)]
    place = lax.broadcasted_iota(jnp.int32, (count, LANES), 0).astype(F32)
    best = jnp.full((count, LANES), HIGH, F32)
    for a, row in zip(above, rows):
        total = jnp.sum(a, axis=0, keepdims=True)
        best = jnp.minimum(best, jnp.where(total <= place, row, HIGH))
    return jnp.min(best, axis=1, keepdims=True)


def as_row(column):
    count = column.shape[0]
    wide = jnp.broadcast_to(column, (count, LANES))
    if count < LANES:
        wide = jnp.concatenate([wide, jnp.full((LANES - count, LANES), -1.0, F32)], axis=0)
    return jnp.transpose(wide)[0:1, :]


def kernel(
    n_pts, n_cand, points, weights, coverage, candidates, picks, gains_out, lists_out, cover_out,
    p_buf, c_buf, w_buf, v_buf, k_buf, w_col, v_col, g_acc, b_acc, part, parts, best, bests,
    top, tops, g_col, in_sem, small_sem, part_send, part_recv, best_send, best_recv, top_send, top_recv,
):
    rows, depth = points.shape
    cands = candidates.shape[0]
    me, mz = lax.axis_index("pts"), lax.axis_index("cand")
    n_p, n_c = rows // CHUNK, cands // CHUNK
    tiles_p, tiles_c = rows // LANES, cands // LANES
    scale = depth ** (-0.5)

    small = [
        pltpu.make_async_copy(weights, w_buf, small_sem.at[0]),
        pltpu.make_async_copy(coverage, v_buf, small_sem.at[1]),
        pltpu.make_async_copy(picks, k_buf, small_sem.at[2]),
    ]
    for copy in small:
        copy.start()
    barrier = pltpu.get_barrier_semaphore()
    for k in range(1, n_cand):
        other = lax.rem(mz + k, n_cand)
        pl.semaphore_signal(barrier, inc=1, device_id={"cand": other}, device_id_type=MESH)
        pl.semaphore_signal(
            barrier, inc=1, device_id={"pts": n_pts - 1, "cand": other}, device_id_type=MESH
        )

    loads = {}
    order = []
    for i in range(max(n_p, n_c)):
        if i < n_c:
            order.append(("c", i))
        if i < n_p:
            order.append(("p", i))
    for at, (kind, i) in enumerate(order):
        src, dst = (points, p_buf) if kind == "p" else (candidates, c_buf)
        span = pl.ds(i * CHUNK, CHUNK)
        loads[kind, i] = pltpu.make_async_copy(src.at[span, :], dst.at[span, :], in_sem.at[at])
        loads[kind, i].start()

    for k in range(1, n_pts):
        pl.semaphore_signal(
            barrier, inc=1, device_id={"pts": lax.rem(me + k, n_pts)}, device_id_type=MESH
        )

    for copy in small:
        copy.wait()
    column = mz * cands + lax.broadcasted_iota(jnp.int32, (tiles_c, LANES), 0) * LANES
    column = column + lax.broadcasted_iota(jnp.int32, (tiles_c, LANES), 1)
    chosen = jnp.zeros((tiles_c, LANES), jnp.bool_)
    for k in range(picks.shape[0]):
        chosen = chosen | (column == k_buf[k])
    penalty = jnp.where(chosen, 0.0, LOW)
    w_row = w_buf[...] * (scale / (rows * n_pts))
    v_row = v_buf[...] * (1.0 / scale)
    for t in range(tiles_p):
        w_col[t * LANES : (t + 1) * LANES, :] = column_tile(w_row[t : t + 1, :])
        v_col[t * LANES : (t + 1) * LANES, :] = column_tile(v_row[t : t + 1, :])

    def block(p_from, p_to, c_from, c_to):
        ps, many = pl.ds(p_from, p_to - p_from), p_to - p_from
        sims = lax.dot_general(
            p_buf[ps, :], c_buf[pl.ds(c_from, c_to - c_from), :],
            (((1,), (1,)), ((), ())), preferred_element_type=F32,
        )
        w, v = w_col[ps, :], v_col[ps, :]
        found = None
        for tile in range(c_from // LANES, c_to // LANES):
            lanes = slice(tile * LANES, (tile + 1) * LANES)
            x = sims[:, tile * LANES - c_from : (tile + 1) * LANES - c_from]
            value = jnp.maximum(x - v, 0.0) * w
            value = jnp.sum(value.reshape(many // 8, 8, LANES), axis=0)
            if p_from == 0:
                g_acc[:, lanes] = value
            else:
                g_acc[:, lanes] += value
            x = x + penalty[tile : tile + 1, :]
            found = x if found is None else jnp.maximum(found, x)
        if c_from == 0:
            b_acc[ps, :] = found
        else:
            b_acc[ps, :] = jnp.maximum(b_acc[ps, :], found)

    here_p = here_c = 0
    for kind, i in order:
        loads[kind, i].wait()
        if kind == "p":
            here_p += CHUNK
            if here_c:
                block(here_p - CHUNK, here_p, 0, here_c)
        else:
            here_c += CHUNK
            if here_p:
                block(0, here_p, here_c - CHUNK, here_c)

    for t in range(tiles_c):
        part[t : t + 1, :] = jnp.sum(g_acc[:, t * LANES : (t + 1) * LANES], axis=0, keepdims=True)

    speaks = me == n_pts - 1
    greetings = n_pts - 1 + n_cand - 1
    pl.semaphore_wait(barrier, jnp.where(speaks, greetings + n_pts * (n_cand - 1), greetings))

    def exchange(axis, n, mine, src, slots, send, recv):
        for k in range(1, n):
            pltpu.make_async_remote_copy(
                src_ref=src, dst_ref=slots.at[mine], send_sem=send.at[k], recv_sem=recv.at[mine],
                device_id={axis: lax.rem(mine + k, n)}, device_id_type=MESH,
            ).start()

    def arrive(axis, n, mine, src, slots, send, recv):
        for k in range(1, n):
            other = lax.rem(mine + k, n)
            pltpu.make_async_remote_copy(
                src_ref=src, dst_ref=slots.at[other], send_sem=send.at[k], recv_sem=recv.at[other],
                device_id={axis: other}, device_id_type=MESH,
            ).wait()

    exchange("pts", n_pts, me, part, parts, part_send, part_recv)
    parts[me] = part[...]

    for t in range(tiles_p):
        turned = jnp.transpose(b_acc[t * LANES : (t + 1) * LANES, :])
        best[t : t + 1, :] = jnp.max(turned, axis=0, keepdims=True)
    exchange("cand", n_cand, mz, best, bests, best_send, best_recv)

    arrive("pts", n_pts, me, part, parts, part_send, part_recv)
    gains = parts[0]
    for k in range(1, n_pts):
        gains = gains + parts[k]
    gains_out[...] = gains

    for t in range(tiles_c):
        g_col[t * LANES : (t + 1) * LANES, :] = column_tile(gains[t : t + 1, :])
    sorted_col = ranked([g_col], [gains[t : t + 1, :] for t in range(tiles_c)], TOPK)
    top_row = as_row(sorted_col)
    top[...] = top_row

    def announce(k, p):
        return pltpu.make_async_remote_copy(
            src_ref=top, dst_ref=tops.at[mz], send_sem=top_send.at[k - 1, p], recv_sem=top_recv.at[mz],
            device_id={"pts": p, "cand": lax.rem(mz + k, n_cand)}, device_id_type=MESH,
        )

    @pl.when(speaks)
    def _():
        for p in range(n_pts):
            for k in range(1, n_cand):
                announce(k, p).start()

    tops[mz] = top_row

    arrive("cand", n_cand, mz, best, bests, best_send, best_recv)
    cover = best[...]
    for k in range(1, n_cand):
        cover = jnp.maximum(cover, bests[lax.rem(mz + k, n_cand)])
    cover_out[...] = jnp.maximum(v_buf[...], cover * scale)

    for k in range(1, n_cand):
        other = lax.rem(mz + k, n_cand)
        pltpu.make_async_remote_copy(
            src_ref=top, dst_ref=tops.at[other], send_sem=top_send.at[0, 0], recv_sem=top_recv.at[other],
            device_id={"pts": n_pts - 1, "cand": other}, device_id_type=MESH,
        ).wait_recv()
    for k in range(n_cand):
        lists_out[k : k + 1, :] = tops[k]

    @pl.when(speaks)
    def _():
        for p in range(n_pts):
            for k in range(1, n_cand):
                announce(k, p).wait_send()


def finish(gains, lists, cover, gains_out, top_out, cover_out, sems, top_buf):
    gains_copy = pltpu.make_async_copy(gains, gains_out, sems.at[0])
    cover_copy = pltpu.make_async_copy(cover, cover_out, sems.at[1])
    gains_copy.start()
    cover_copy.start()
    rows = [lists[k : k + 1, :] for k in range(lists.shape[0])]
    merged = ranked([column_tile(row)[:TOPK, :] for row in rows], rows, TOPK)
    top_buf[...] = as_row(merged)[:, :TOPK]
    top_copy = pltpu.make_async_copy(top_buf, top_out, sems.at[2])
    top_copy.start()
    gains_copy.wait()
    cover_copy.wait()
    top_copy.wait()


def solution(mesh):
    n_pts, n_cand = mesh.shape["pts"], mesh.shape["cand"]

    def on_device(points, weights, coverage, candidates, picks):
        rows, depth = points.shape
        cands = candidates.shape[0]
        tp, tc = rows // LANES, cands // LANES
        anywhere = pl.BlockSpec(memory_space=pl.ANY)
        dma = pltpu.SemaphoreType.DMA
        vmem = pltpu.VMEM
        gains, lists, cover = pl.pallas_call(
            functools.partial(kernel, n_pts, n_cand),
            out_shape=(
                vmem((tc, LANES), F32),
                vmem((n_cand, LANES), F32),
                vmem((tp, LANES), F32),
            ),
            in_specs=[anywhere] * 5,
            out_specs=(pl.BlockSpec(memory_space=vmem),) * 3,
            scratch_shapes=[
                vmem((rows, depth), points.dtype), vmem((cands, depth), candidates.dtype),
                vmem((tp, LANES), F32), vmem((tp, LANES), F32),
                pltpu.SMEM(picks.shape, jnp.int32),
                vmem((rows, LANES), F32), vmem((rows, LANES), F32),
                vmem((8, cands), F32), vmem((rows, LANES), F32),
                vmem((tc, LANES), F32), vmem((n_pts, tc, LANES), F32),
                vmem((tp, LANES), F32), vmem((n_cand, tp, LANES), F32),
                vmem((1, LANES), F32), vmem((n_cand, 1, LANES), F32),
                vmem((cands, LANES), F32),
                dma((rows // CHUNK + cands // CHUNK,)), dma((3,)),
                dma((n_pts,)), dma((n_pts,)),
                dma((n_cand,)), dma((n_cand,)),
                dma((n_cand - 1, n_pts)), dma((n_cand,)),
            ],
            compiler_params=pltpu.CompilerParams(
                collective_id=0, has_side_effects=True, vmem_limit_bytes=60 * 2**20
            ),
            name="facility",
        )(points, weights.reshape(tp, LANES), coverage.reshape(tp, LANES), candidates, picks)
        gains, top, cover = pl.pallas_call(
            finish,
            out_shape=(
                jax.ShapeDtypeStruct((tc, LANES), F32),
                jax.ShapeDtypeStruct((1, TOPK), F32),
                jax.ShapeDtypeStruct((tp, LANES), F32),
            ),
            in_specs=[pl.BlockSpec(memory_space=vmem)] * 3,
            out_specs=(anywhere,) * 3,
            scratch_shapes=[dma((3,)), vmem((1, TOPK), F32)],
            name="finish",
        )(*(pltpu.with_memory_space_constraint(x, vmem) for x in (gains, lists, cover)))
        return gains.reshape(cands), top.reshape(TOPK), cover.reshape(rows)

    placed = (P("pts", None), P("pts"), P("pts"), P("cand", None), P())
    return jax.shard_map(
        on_device, mesh=mesh, in_specs=placed, out_specs=(P("cand"), P(), P("pts")), check_vma=False
    )
```

```python
import functools

import jax
import jax.numpy as jnp
from jax import lax
from jax.experimental import pallas as pl
from jax.experimental.pallas import tpu as pltpu
from jax.sharding import PartitionSpec as P

TOPK = 64
LANES = 128
MESH = pl.DeviceIdType.MESH
F32 = jnp.float32
LOW = -1e30
HIGH = 3e38
CHUNK = 256


def column_tile(row):
    return jnp.transpose(jnp.broadcast_to(row, (LANES, LANES)))


def ranked(columns, rows, count):
    wide = [jnp.broadcast_to(row, (8, LANES)) for row in rows]
    above = [jnp.zeros((8, LANES), F32) for _ in rows]
    for column in columns:
        for g in range(column.shape[0] // 8):
            value = column[g * 8 : (g + 1) * 8, :]
            above = [a + jnp.where(value > w, 1.0, 0.0) for a, w in zip(above, wide)]
    place = lax.broadcasted_iota(jnp.int32, (count, LANES), 0).astype(F32)
    best = jnp.full((count, LANES), HIGH, F32)
    for a, row in zip(above, rows):
        total = jnp.sum(a, axis=0, keepdims=True)
        best = jnp.minimum(best, jnp.where(total <= place, row, HIGH))
    return jnp.min(best, axis=1, keepdims=True)


def as_row(column):
    count = column.shape[0]
    wide = jnp.broadcast_to(column, (count, LANES))
    if count < LANES:
        wide = jnp.concatenate([wide, jnp.full((LANES - count, LANES), -1.0, F32)], axis=0)
    return jnp.transpose(wide)[0:1, :]


def kernel(
    n_pts, n_cand, points, weights, coverage, candidates, picks, gains_out, lists_out, cover_out,
    p_buf, c_buf, w_buf, v_buf, k_buf, w_col, v_col, g_acc, b_acc, part, parts, best, bests,
    top, tops, g_col, in_sem, small_sem, part_send, part_recv, best_send, best_recv, top_send, top_recv,
    spoken,
):
    rows, depth = points.shape
    cands = candidates.shape[0]
    me, mz = lax.axis_index("pts"), lax.axis_index("cand")
    n_p, n_c = rows // CHUNK, cands // CHUNK
    tiles_p, tiles_c = rows // LANES, cands // LANES
    scale = depth ** (-0.5)

    small = [
        pltpu.make_async_copy(weights, w_buf, small_sem.at[0]),
        pltpu.make_async_copy(coverage, v_buf, small_sem.at[1]),
        pltpu.make_async_copy(picks, k_buf, small_sem.at[2]),
    ]
    for copy in small:
        copy.start()
    barrier = pltpu.get_barrier_semaphore()
    for k in range(1, n_cand):
        other = lax.rem(mz + k, n_cand)
        pl.semaphore_signal(barrier, inc=1, device_id={"cand": other}, device_id_type=MESH)
        pl.semaphore_signal(
            barrier, inc=1, device_id={"pts": n_pts - 1, "cand": other}, device_id_type=MESH
        )

    loads = {}
    order = []
    for i in range(max(n_p, n_c)):
        if i < n_c:
            order.append(("c", i))
        if i < n_p:
            order.append(("p", i))
    for at, (kind, i) in enumerate(order):
        src, dst = (points, p_buf) if kind == "p" else (candidates, c_buf)
        span = pl.ds(i * CHUNK, CHUNK)
        loads[kind, i] = pltpu.make_async_copy(src.at[span, :], dst.at[span, :], in_sem.at[at])
        loads[kind, i].start()

    for k in range(1, n_pts):
        pl.semaphore_signal(
            barrier, inc=1, device_id={"pts": lax.rem(me + k, n_pts)}, device_id_type=MESH
        )

    for copy in small:
        copy.wait()
    column = mz * cands + lax.broadcasted_iota(jnp.int32, (tiles_c, LANES), 0) * LANES
    column = column + lax.broadcasted_iota(jnp.int32, (tiles_c, LANES), 1)
    chosen = jnp.zeros((tiles_c, LANES), jnp.bool_)
    for k in range(picks.shape[0]):
        chosen = chosen | (column == k_buf[k])
    penalty = jnp.where(chosen, 0.0, LOW)
    w_row = w_buf[...] * (scale / (rows * n_pts))
    v_row = v_buf[...] * (1.0 / scale)
    for t in range(tiles_p):
        w_col[t * LANES : (t + 1) * LANES, :] = column_tile(w_row[t : t + 1, :])
        v_col[t * LANES : (t + 1) * LANES, :] = column_tile(v_row[t : t + 1, :])

    def block(p_from, p_to, c_from, c_to):
        ps, many = pl.ds(p_from, p_to - p_from), p_to - p_from
        sims = lax.dot_general(
            p_buf[ps, :], c_buf[pl.ds(c_from, c_to - c_from), :],
            (((1,), (1,)), ((), ())), preferred_element_type=F32,
        )
        w, v = w_col[ps, :], v_col[ps, :]
        found = None
        for tile in range(c_from // LANES, c_to // LANES):
            lanes = slice(tile * LANES, (tile + 1) * LANES)
            x = sims[:, tile * LANES - c_from : (tile + 1) * LANES - c_from]
            value = jnp.maximum(x - v, 0.0) * w
            value = jnp.sum(value.reshape(many // 8, 8, LANES), axis=0)
            if p_from == 0:
                g_acc[:, lanes] = value
            else:
                g_acc[:, lanes] += value
            x = x + penalty[tile : tile + 1, :]
            found = x if found is None else jnp.maximum(found, x)
        if c_from == 0:
            b_acc[ps, :] = found
        else:
            b_acc[ps, :] = jnp.maximum(b_acc[ps, :], found)

    here_p = here_c = 0
    for kind, i in order:
        loads[kind, i].wait()
        if kind == "p":
            here_p += CHUNK
            if here_c:
                block(here_p - CHUNK, here_p, 0, here_c)
        else:
            here_c += CHUNK
            if here_p:
                block(0, here_p, here_c - CHUNK, here_c)

    for t in range(tiles_c):
        part[t : t + 1, :] = jnp.sum(g_acc[:, t * LANES : (t + 1) * LANES], axis=0, keepdims=True)

    speaks = me == n_pts - 1
    greetings = n_pts - 1 + n_cand - 1
    pl.semaphore_wait(barrier, jnp.where(speaks, greetings + n_pts * (n_cand - 1), greetings))

    def exchange(axis, n, mine, src, slots, send, recv):
        for k in range(1, n):
            pltpu.make_async_remote_copy(
                src_ref=src, dst_ref=slots.at[mine], send_sem=send.at[0], recv_sem=recv.at[0],
                device_id={axis: lax.rem(mine + k, n)}, device_id_type=MESH,
            ).start()

    def settle(slots, n, sem):
        view = slots.at[pl.ds(0, n)]
        pltpu.make_async_copy(view, view, sem.at[0]).wait()

    exchange("pts", n_pts, me, part, parts, part_send, part_recv)
    parts[me] = part[...]

    def cover_exchange():
        for t in range(tiles_p):
            turned = jnp.transpose(b_acc[t * LANES : (t + 1) * LANES, :])
            best[t : t + 1, :] = jnp.max(turned, axis=0, keepdims=True)
        exchange("cand", n_cand, mz, best, bests, best_send, best_recv)

    pl.when(jnp.logical_not(speaks))(cover_exchange)

    settle(parts, n_pts - 1, part_recv)
    gains = parts[0]
    for k in range(1, n_pts):
        gains = gains + parts[k]
    gains_out[...] = gains

    for t in range(tiles_c):
        g_col[t * LANES : (t + 1) * LANES, :] = column_tile(gains[t : t + 1, :])
    sorted_col = ranked([g_col], [gains[t : t + 1, :] for t in range(tiles_c)], TOPK)
    top_row = as_row(sorted_col)
    top[...] = top_row

    def announce(k, p):
        return pltpu.make_async_remote_copy(
            src_ref=top, dst_ref=tops.at[mz], send_sem=top_send.at[0], recv_sem=top_recv.at[0],
            device_id={"pts": p, "cand": lax.rem(mz + k, n_cand)}, device_id_type=MESH,
        )

    @pl.when(speaks)
    def _():
        for p in range(n_pts):
            for k in range(1, n_cand):
                announce(k, p).start()
        cover_exchange()

    tops[mz] = top_row

    settle(bests, n_cand - 1, best_recv)
    cover = best[...]
    for k in range(1, n_cand):
        cover = jnp.maximum(cover, bests[lax.rem(mz + k, n_cand)])
    cover_out[...] = jnp.maximum(v_buf[...], cover * scale)

    settle(tops, n_cand - 1, top_recv)
    for k in range(n_cand):
        lists_out[k : k + 1, :] = tops[k]

    settle(parts, n_pts - 1, part_send)
    settle(bests, n_cand - 1, best_send)

    @pl.when(speaks)
    def _():
        settle(spoken, n_pts * (n_cand - 1), top_send)


def finish(gains, lists, cover, gains_out, top_out, cover_out, sems, top_buf):
    gains_copy = pltpu.make_async_copy(gains, gains_out, sems.at[0])
    cover_copy = pltpu.make_async_copy(cover, cover_out, sems.at[1])
    gains_copy.start()
    cover_copy.start()
    rows = [lists[k : k + 1, :] for k in range(lists.shape[0])]
    merged = ranked([column_tile(row)[:TOPK, :] for row in rows], rows, TOPK)
    top_buf[...] = as_row(merged)[:, :TOPK]
    top_copy = pltpu.make_async_copy(top_buf, top_out, sems.at[2])
    top_copy.start()
    gains_copy.wait()
    cover_copy.wait()
    top_copy.wait()


def solution(mesh):
    n_pts, n_cand = mesh.shape["pts"], mesh.shape["cand"]

    def on_device(points, weights, coverage, candidates, picks):
        rows, depth = points.shape
        cands = candidates.shape[0]
        tp, tc = rows // LANES, cands // LANES
        anywhere = pl.BlockSpec(memory_space=pl.ANY)
        dma = pltpu.SemaphoreType.DMA
        vmem = pltpu.VMEM
        gains, lists, cover = pl.pallas_call(
            functools.partial(kernel, n_pts, n_cand),
            out_shape=(
                vmem((tc, LANES), F32),
                vmem((n_cand, LANES), F32),
                vmem((tp, LANES), F32),
            ),
            in_specs=[anywhere] * 5,
            out_specs=(pl.BlockSpec(memory_space=vmem),) * 3,
            scratch_shapes=[
                vmem((rows, depth), points.dtype), vmem((cands, depth), candidates.dtype),
                vmem((tp, LANES), F32), vmem((tp, LANES), F32),
                pltpu.SMEM(picks.shape, jnp.int32),
                vmem((rows, LANES), F32), vmem((rows, LANES), F32),
                vmem((8, cands), F32), vmem((rows, LANES), F32),
                vmem((tc, LANES), F32), vmem((n_pts, tc, LANES), F32),
                vmem((tp, LANES), F32), vmem((n_cand, tp, LANES), F32),
                vmem((1, LANES), F32), vmem((n_cand, 1, LANES), F32),
                vmem((cands, LANES), F32),
                dma((rows // CHUNK + cands // CHUNK,)), dma((3,)),
                dma((1,)), dma((1,)), dma((1,)), dma((1,)), dma((1,)), dma((1,)),
                vmem((n_pts * (n_cand - 1), 1, LANES), F32),
            ],
            compiler_params=pltpu.CompilerParams(
                collective_id=0, has_side_effects=True, vmem_limit_bytes=60 * 2**20
            ),
            name="facility",
        )(points, weights.reshape(tp, LANES), coverage.reshape(tp, LANES), candidates, picks)
        gains, top, cover = pl.pallas_call(
            finish,
            out_shape=(
                jax.ShapeDtypeStruct((tc, LANES), F32),
                jax.ShapeDtypeStruct((1, TOPK), F32),
                jax.ShapeDtypeStruct((tp, LANES), F32),
            ),
            in_specs=[pl.BlockSpec(memory_space=vmem)] * 3,
            out_specs=(anywhere,) * 3,
            scratch_shapes=[dma((3,)), vmem((1, TOPK), F32)],
            name="finish",
        )(*(pltpu.with_memory_space_constraint(x, vmem) for x in (gains, lists, cover)))
        return gains.reshape(cands), top.reshape(TOPK), cover.reshape(rows)

    placed = (P("pts", None), P("pts"), P("pts"), P("cand", None), P())
    return jax.shard_map(
        on_device, mesh=mesh, in_specs=placed, out_specs=(P("cand"), P(), P("pts")), check_vma=False
    )
```

```python
import functools

import jax
import jax.numpy as jnp
from jax import lax
from jax.experimental import pallas as pl
from jax.experimental.pallas import tpu as pltpu
from jax.sharding import PartitionSpec as P

TOPK = 64
LANES = 128
MESH = pl.DeviceIdType.MESH
F32 = jnp.float32
LOW = -1e30
HIGH = 3e38
CHUNK = 512


def column_tile(row):
    return jnp.transpose(jnp.broadcast_to(row, (LANES, LANES)))


def ranked(columns, rows, count):
    wide = [jnp.broadcast_to(row, (8, LANES)) for row in rows]
    above = [jnp.zeros((8, LANES), F32) for _ in rows]
    for column in columns:
        for g in range(column.shape[0] // 8):
            value = column[g * 8 : (g + 1) * 8, :]
            above = [a + jnp.where(value > w, 1.0, 0.0) for a, w in zip(above, wide)]
    place = lax.broadcasted_iota(jnp.int32, (count, LANES), 0).astype(F32)
    best = jnp.full((count, LANES), HIGH, F32)
    for a, row in zip(above, rows):
        total = jnp.sum(a, axis=0, keepdims=True)
        best = jnp.minimum(best, jnp.where(total <= place, row, HIGH))
    return jnp.min(best, axis=1, keepdims=True)


def as_row(column):
    count = column.shape[0]
    wide = jnp.broadcast_to(column, (count, LANES))
    if count < LANES:
        wide = jnp.concatenate([wide, jnp.full((LANES - count, LANES), -1.0, F32)], axis=0)
    return jnp.transpose(wide)[0:1, :]


def kernel(
    n_pts, n_cand, points, weights, coverage, candidates, picks, gains_out, lists_out, cover_out,
    p_buf, c_buf, w_buf, v_buf, k_buf, w_col, v_col, g_acc, b_acc, part, parts, best, bests,
    top, tops, g_col, in_sem, small_sem, part_send, part_recv, best_send, best_recv, top_send, top_recv,
    spoken,
):
    rows, depth = points.shape
    cands = candidates.shape[0]
    me, mz = lax.axis_index("pts"), lax.axis_index("cand")
    n_p, n_c = rows // CHUNK, cands // CHUNK
    tiles_p, tiles_c = rows // LANES, cands // LANES
    scale = depth ** (-0.5)

    small = [
        pltpu.make_async_copy(weights, w_buf, small_sem.at[0]),
        pltpu.make_async_copy(coverage, v_buf, small_sem.at[1]),
        pltpu.make_async_copy(picks, k_buf, small_sem.at[2]),
    ]
    for copy in small:
        copy.start()
    barrier = pltpu.get_barrier_semaphore()
    for k in range(1, n_cand):
        other = lax.rem(mz + k, n_cand)
        pl.semaphore_signal(barrier, inc=1, device_id={"cand": other}, device_id_type=MESH)
        pl.semaphore_signal(
            barrier, inc=1, device_id={"pts": n_pts - 1, "cand": other}, device_id_type=MESH
        )

    loads = {}
    order = []
    for i in range(max(n_p, n_c)):
        if i < n_c:
            order.append(("c", i))
        if i < n_p:
            order.append(("p", i))
    for at, (kind, i) in enumerate(order):
        src, dst = (points, p_buf) if kind == "p" else (candidates, c_buf)
        span = pl.ds(i * CHUNK, CHUNK)
        loads[kind, i] = pltpu.make_async_copy(src.at[span, :], dst.at[span, :], in_sem.at[at])
        loads[kind, i].start()

    for k in range(1, n_pts):
        pl.semaphore_signal(
            barrier, inc=1, device_id={"pts": lax.rem(me + k, n_pts)}, device_id_type=MESH
        )

    for copy in small:
        copy.wait()
    column = mz * cands + lax.broadcasted_iota(jnp.int32, (tiles_c, LANES), 0) * LANES
    column = column + lax.broadcasted_iota(jnp.int32, (tiles_c, LANES), 1)
    chosen = jnp.zeros((tiles_c, LANES), jnp.bool_)
    for k in range(picks.shape[0]):
        chosen = chosen | (column == k_buf[k])
    penalty = jnp.where(chosen, 0.0, LOW)
    w_row = w_buf[...] * (scale / (rows * n_pts))
    v_row = v_buf[...] * (1.0 / scale)
    for t in range(tiles_p):
        w_col[t * LANES : (t + 1) * LANES, :] = column_tile(w_row[t : t + 1, :])
        v_col[t * LANES : (t + 1) * LANES, :] = column_tile(v_row[t : t + 1, :])

    def block(p_from, p_to, c_from, c_to):
        ps, many = pl.ds(p_from, p_to - p_from), p_to - p_from
        sims = lax.dot_general(
            p_buf[ps, :], c_buf[pl.ds(c_from, c_to - c_from), :],
            (((1,), (1,)), ((), ())), preferred_element_type=F32,
        )
        w, v = w_col[ps, :], v_col[ps, :]
        found = None
        for tile in range(c_from // LANES, c_to // LANES):
            lanes = slice(tile * LANES, (tile + 1) * LANES)
            x = sims[:, tile * LANES - c_from : (tile + 1) * LANES - c_from]
            value = jnp.maximum(x - v, 0.0) * w
            value = jnp.sum(value.reshape(many // 8, 8, LANES), axis=0)
            if p_from == 0:
                g_acc[:, lanes] = value
            else:
                g_acc[:, lanes] += value
            x = x + penalty[tile : tile + 1, :]
            found = x if found is None else jnp.maximum(found, x)
        if c_from == 0:
            b_acc[ps, :] = found
        else:
            b_acc[ps, :] = jnp.maximum(b_acc[ps, :], found)

    here_p = here_c = 0
    for kind, i in order:
        loads[kind, i].wait()
        if kind == "p":
            here_p += CHUNK
            if here_c:
                block(here_p - CHUNK, here_p, 0, here_c)
        else:
            here_c += CHUNK
            if here_p:
                block(0, here_p, here_c - CHUNK, here_c)

    for t in range(tiles_c):
        part[t : t + 1, :] = jnp.sum(g_acc[:, t * LANES : (t + 1) * LANES], axis=0, keepdims=True)

    speaks = me == n_pts - 1
    greetings = n_pts - 1 + n_cand - 1
    pl.semaphore_wait(barrier, jnp.where(speaks, greetings + n_pts * (n_cand - 1), greetings))

    def exchange(axis, n, mine, src, slots, send, recv):
        for k in range(1, n):
            pltpu.make_async_remote_copy(
                src_ref=src, dst_ref=slots.at[mine], send_sem=send.at[0], recv_sem=recv.at[0],
                device_id={axis: lax.rem(mine + k, n)}, device_id_type=MESH,
            ).start()

    def settle(slots, n, sem):
        view = slots.at[pl.ds(0, n)]
        pltpu.make_async_copy(view, view, sem.at[0]).wait()

    exchange("pts", n_pts, me, part, parts, part_send, part_recv)
    parts[me] = part[...]

    def cover_exchange():
        for t in range(tiles_p):
            turned = jnp.transpose(b_acc[t * LANES : (t + 1) * LANES, :])
            best[t : t + 1, :] = jnp.max(turned, axis=0, keepdims=True)
        exchange("cand", n_cand, mz, best, bests, best_send, best_recv)

    pl.when(jnp.logical_not(speaks))(cover_exchange)

    settle(parts, n_pts - 1, part_recv)
    gains = parts[0]
    for k in range(1, n_pts):
        gains = gains + parts[k]
    gains_out[...] = gains

    for t in range(tiles_c):
        g_col[t * LANES : (t + 1) * LANES, :] = column_tile(gains[t : t + 1, :])
    sorted_col = ranked([g_col], [gains[t : t + 1, :] for t in range(tiles_c)], TOPK)
    top_row = as_row(sorted_col)
    top[...] = top_row

    def announce(k, p):
        return pltpu.make_async_remote_copy(
            src_ref=top, dst_ref=tops.at[mz], send_sem=top_send.at[0], recv_sem=top_recv.at[0],
            device_id={"pts": p, "cand": lax.rem(mz + k, n_cand)}, device_id_type=MESH,
        )

    @pl.when(speaks)
    def _():
        for p in range(n_pts):
            for k in range(1, n_cand):
                announce(k, p).start()
        cover_exchange()

    tops[mz] = top_row

    settle(bests, n_cand - 1, best_recv)
    cover = best[...]
    for k in range(1, n_cand):
        cover = jnp.maximum(cover, bests[lax.rem(mz + k, n_cand)])
    cover_out[...] = jnp.maximum(v_buf[...], cover * scale)

    settle(tops, n_cand - 1, top_recv)
    for k in range(n_cand):
        lists_out[k : k + 1, :] = tops[k]

    settle(parts, n_pts - 1, part_send)
    settle(bests, n_cand - 1, best_send)

    @pl.when(speaks)
    def _():
        settle(spoken, n_pts * (n_cand - 1), top_send)


def finish(gains, lists, cover, gains_out, top_out, cover_out, sems, top_buf):
    gains_copy = pltpu.make_async_copy(gains, gains_out, sems.at[0])
    cover_copy = pltpu.make_async_copy(cover, cover_out, sems.at[1])
    gains_copy.start()
    cover_copy.start()
    rows = [lists[k : k + 1, :] for k in range(lists.shape[0])]
    merged = ranked([column_tile(row)[:TOPK, :] for row in rows], rows, TOPK)
    top_buf[...] = as_row(merged)[:, :TOPK]
    top_copy = pltpu.make_async_copy(top_buf, top_out, sems.at[2])
    top_copy.start()
    gains_copy.wait()
    cover_copy.wait()
    top_copy.wait()


def solution(mesh):
    n_pts, n_cand = mesh.shape["pts"], mesh.shape["cand"]

    def on_device(points, weights, coverage, candidates, picks):
        rows, depth = points.shape
        cands = candidates.shape[0]
        tp, tc = rows // LANES, cands // LANES
        anywhere = pl.BlockSpec(memory_space=pl.ANY)
        dma = pltpu.SemaphoreType.DMA
        vmem = pltpu.VMEM
        gains, lists, cover = pl.pallas_call(
            functools.partial(kernel, n_pts, n_cand),
            out_shape=(
                vmem((tc, LANES), F32),
                vmem((n_cand, LANES), F32),
                vmem((tp, LANES), F32),
            ),
            in_specs=[anywhere] * 5,
            out_specs=(pl.BlockSpec(memory_space=vmem),) * 3,
            scratch_shapes=[
                vmem((rows, depth), points.dtype), vmem((cands, depth), candidates.dtype),
                vmem((tp, LANES), F32), vmem((tp, LANES), F32),
                pltpu.SMEM(picks.shape, jnp.int32),
                vmem((rows, LANES), F32), vmem((rows, LANES), F32),
                vmem((8, cands), F32), vmem((rows, LANES), F32),
                vmem((tc, LANES), F32), vmem((n_pts, tc, LANES), F32),
                vmem((tp, LANES), F32), vmem((n_cand, tp, LANES), F32),
                vmem((1, LANES), F32), vmem((n_cand, 1, LANES), F32),
                vmem((cands, LANES), F32),
                dma((rows // CHUNK + cands // CHUNK,)), dma((3,)),
                dma((1,)), dma((1,)), dma((1,)), dma((1,)), dma((1,)), dma((1,)),
                vmem((n_pts * (n_cand - 1), 1, LANES), F32),
            ],
            compiler_params=pltpu.CompilerParams(
                collective_id=0, has_side_effects=True, vmem_limit_bytes=60 * 2**20
            ),
            name="facility",
        )(points, weights.reshape(tp, LANES), coverage.reshape(tp, LANES), candidates, picks)
        gains, top, cover = pl.pallas_call(
            finish,
            out_shape=(
                jax.ShapeDtypeStruct((tc, LANES), F32),
                jax.ShapeDtypeStruct((1, TOPK), F32),
                jax.ShapeDtypeStruct((tp, LANES), F32),
            ),
            in_specs=[pl.BlockSpec(memory_space=vmem)] * 3,
            out_specs=(anywhere,) * 3,
            scratch_shapes=[dma((3,)), vmem((1, TOPK), F32)],
            name="finish",
        )(*(pltpu.with_memory_space_constraint(x, vmem) for x in (gains, lists, cover)))
        return gains.reshape(cands), top.reshape(TOPK), cover.reshape(rows)

    placed = (P("pts", None), P("pts"), P("pts"), P("cand", None), P())
    return jax.shard_map(
        on_device, mesh=mesh, in_specs=placed, out_specs=(P("cand"), P(), P("pts")), check_vma=False
    )
```
